32 devices in a mesh: tm: 8 (over z, y), mp: 4 (over x, core).
Axes of the slice: x: 2, y: 2, z: 4, core: 2. Of those that a mesh axis runs over, the one named last changes fastest.
Arguments:
- latents: float32 [4, 8, 4, 4096], P(None, 'tm'), may hold values from -6 to 6
- noise: float32 [4, 8, 4, 4096], P(None, 'tm'), may hold values from -6 to 6
- start_step: int32 [4], replicated, may hold values from 8 to 999
- slide: int32 [4], replicated, may hold values from 1 to 8, as said below
- w_in: float32 [4, 320], replicated, may hold values from -3 to 3
- w_gate: bfloat16 [320, 1280], P(None, 'mp'), may hold values from -0.3125 to 0.3125
- w_value: bfloat16 [320, 1280], P(None, 'mp'), may hold values from -0.3125 to 0.3125
- w_down: bfloat16 [1280, 320], P('mp'), may hold values from -0.15625 to 0.15625
- w_out: float32 [320, 4], replicated, may hold values from -0.3125 to 0.3125
Outputs:
- next_window: float32 [4, 8, 4, 4096], P(None, 'tm')
- eps: float32 [4, 8, 4, 4096], P(None, 'tm', None, 'mp')
The draws below stay inside these ranges and needn't reach their ends.
Inputs may be any that keep to these rules, and one draw needn't show every extreme that they name: `slide`: some prompt slides by exactly 8, and another by exactly 1.
All inputs are finite; a program needn't handle non-finite values.
Results may differ from the reference program's by a relative error of at most 0.0023.
Values sent between devices are 32-bit elements; how exact they have to be, the bound alone decides.
A program may use at most 64 MiB of HBM per device.

```python
import math
import jax
import jax.numpy as jnp
from jax import lax

C = 320
FF = 1280
LAT = 4
POS = 4096
PROMPTS = 4
TSTEPS = 1000
WIN = 8
SMAX = 8


def draw_slide(key, part):
    first, second = jax.random.split(jax.random.fold_in(key, 17))
    values = jax.random.randint(first, (PROMPTS,), 1, SMAX + 1)
    order = jax.random.permutation(second, PROMPTS)
    values = jnp.where(order == 0, SMAX, values)
    values = jnp.where(order == 1, 1, values)
    return values.astype(jnp.int32)


def plant(array, own_key, low, top_value):
    longest = array.shape.index(max(array.shape))
    spots = []
    for shift in (0, 1):
        where = [jax.random.randint(jax.random.fold_in(own_key, axis), (), 0, length) for axis, length in enumerate(array.shape)]
        where[longest] = (where[longest] + shift) % array.shape[longest]
        spots.append(tuple(where))
    return array.at[spots[0]].set(low).at[spots[1]].set(top_value)


def block_levels(key, dims, cuts, least, largest):
    level, own = 1.0, jax.random.fold_in(key, 6)
    for position, shards_of in cuts:
        steps = jnp.exp(jax.random.uniform(jax.random.fold_in(own, position), (shards_of,), jnp.float32, least / len(cuts), largest / len(cuts)))
        level = level * jnp.repeat(steps, dims[position] // shards_of).reshape([-1 if axis == position else 1 for axis in range(len(dims))])
    return level


def bell_draw(rng, extent, deviation, bound, pieces=(), kind=jnp.bfloat16):
    loudness = block_levels(rng, extent, pieces, -0.22, 0.18) if pieces else 1.0
    entries = jax.random.normal(rng, extent, jnp.float32) * deviation * loudness
    return jnp.minimum(jnp.maximum(entries, -bound), bound).astype(kind)


def setup_inputs(seed: int = 0) -> dict:
    splits = jax.random.split(jax.random.key(seed), 10)
    latents = bell_draw(splits[0], (PROMPTS, WIN, LAT, POS), 1.0, 6.0, ((1, 8),), jnp.float32)
    noise = bell_draw(splits[1], (PROMPTS, WIN, LAT, POS), 1.0, 6.0, ((1, 8),), jnp.float32)
    start_step = plant(jax.random.randint(splits[2], (PROMPTS,), WIN, TSTEPS), jax.random.fold_in(splits[2], 1), WIN, TSTEPS - 1).astype(jnp.int32)
    slide = draw_slide(jax.random.fold_in(splits[9], 71), 0)
    w_in = bell_draw(splits[4], (LAT, C), LAT ** -0.5, 3.0, (), jnp.float32)
    w_gate = bell_draw(splits[5], (C, FF), C ** -0.5, 0.3125, ((1, 4),))
    w_value = bell_draw(splits[6], (C, FF), C ** -0.5, 0.3125, ((1, 4),))
    w_down = bell_draw(splits[7], (FF, C), FF ** -0.5, 0.15625, ((0, 4),))
    w_out = bell_draw(splits[8], (C, LAT), C ** -0.5, 0.3125, (), jnp.float32)
    return {"latents": latents, "noise": noise, "start_step": start_step, "slide": slide, "w_in": w_in, "w_gate": w_gate, "w_value": w_value, "w_down": w_down, "w_out": w_out}


def plan():
    steps_f = jnp.arange(TSTEPS, dtype=jnp.float32)
    beta = 0.0001 + (0.02 - 0.0001) * steps_f / (TSTEPS - 1)
    abar = jnp.cumprod(1.0 - beta)
    return (beta, abar)

def embed(times):
    half = C // 2
    freq = jnp.exp(-math.log(10000.0) * jnp.arange(half, dtype=jnp.float32) / half)
    angle = times[..., None] * freq
    return jnp.concatenate([jnp.cos(angle), jnp.sin(angle)], axis=-1)

def reference(latents, noise, start_step, slide, w_in, w_gate, w_value, w_down, w_out):
    beta, abar = plan()
    slots = jnp.arange(WIN, dtype=jnp.int32)
    times = start_step[:, None] - slots[None, :]
    beta_t = beta[times][:, :, None, None]
    abar_t = abar[times][:, :, None, None]
    emb = embed(times.astype(jnp.float32)).reshape(PROMPTS * WIN, C)
    items = latents.reshape(PROMPTS * WIN, LAT, POS)

    def denoise(pair):
        latent, vector = pair
        hid = jnp.dot(w_in.T, latent, precision=lax.Precision.HIGHEST) + vector[:, None]
        mean = lax.optimization_barrier(jnp.mean(hid, axis=0))
        var = lax.optimization_barrier(jnp.mean((hid - mean) ** 2, axis=0))
        normed = ((hid - mean) * lax.rsqrt(var + 1e-05)).astype(jnp.bfloat16)
        gate = jnp.dot(w_gate.T, normed, preferred_element_type=jnp.float32)
        value = jnp.dot(w_value.T, normed, preferred_element_type=jnp.float32)
        hidden = (jax.nn.gelu(gate, approximate=False) * value).astype(jnp.bfloat16)
        branch = jnp.dot(w_down.T, hidden, preferred_element_type=jnp.float32)
        return jnp.dot(w_out.T, hid + branch, precision=lax.Precision.HIGHEST)
    eps = lax.map(denoise, (items, emb)).reshape(PROMPTS, WIN, LAT, POS)
    stepped = (latents - beta_t / jnp.sqrt(1.0 - abar_t) * eps) / jnp.sqrt(1.0 - beta_t) + jnp.sqrt(beta_t) * noise
    drift = stepped - latents
    updated = latents[:, :1] + (jnp.cumsum(drift, axis=1) - drift)
    source = jnp.minimum(slots[None, :] + slide[:, None], WIN - 1).astype(jnp.int32)
    next_window = jnp.take_along_axis(updated, source[:, :, None, None], axis=1)
    return (next_window, eps)
```

```python
import functools
import math

import jax
import jax.numpy as jnp
import numpy as np
from jax import lax
from jax.experimental import pallas as pl
from jax.experimental.pallas import tpu as pltpu
from jax.sharding import PartitionSpec as P

TSTEPS = 1000
F32, BF16 = jnp.float32, jnp.bfloat16
HIGH = lax.Precision.HIGHEST


def step_table():
    beta = 1e-4 + (0.02 - 1e-4) * np.arange(TSTEPS, dtype=np.float64) / (TSTEPS - 1)
    abar = np.cumprod(1.0 - beta)
    root = np.sqrt(1.0 - beta)
    return np.stack([1.0 / root - 1.0, beta / np.sqrt(1.0 - abar) / root, np.sqrt(beta)]).astype(np.float32)


def embed(times, channels):
    half = channels // 2
    freq = jnp.exp(-math.log(10000.0) * jnp.arange(half, dtype=F32) / half)
    angle = times[..., None] * freq
    return jnp.concatenate([jnp.cos(angle), jnp.sin(angle)], axis=-1)


def split3(v):
    a = v.astype(BF16).astype(F32)
    rest = v - a
    b = rest.astype(BF16).astype(F32)
    return a, b, rest - b


def contract(a, b, da, db, **kw):
    return lax.dot_general(a, b, (((da,), (db,)), ((), ())), preferred_element_type=F32, **kw)


def kernel(n_tm, n_mp, tile, x_ref, z_ref, emb_ref, scal_ref, win_ref, wg_ref, wv_ref, wd_ref, wo_ref,
           out_ref, eps_ref, wbuf, a_scr, f_scr, y_scr, acc, dbuf,
           wsend, wrecv, dsend, drecv, osend, orecv):
    prompts, _, lat, pos = x_ref.shape
    units = wg_ref.shape[1]
    rank = lat + prompts
    share = pos // n_mp
    tm, mp = lax.axis_index("tm"), lax.axis_index("mp")
    cols = pl.ds(pl.multiple_of(mp * share, 128), share)

    barrier = pltpu.get_barrier_semaphore()

    def greet_tm(k, _):
        pl.semaphore_signal(barrier, inc=1, device_id={"tm": lax.rem(tm + k, n_tm)}, device_id_type=pl.DeviceIdType.MESH)
        return 0

    lax.fori_loop(1, n_tm, greet_tm, 0)
    for k in range(1, n_mp):
        pl.semaphore_signal(barrier, inc=1, device_id={"mp": lax.rem(mp + k, n_mp)}, device_id_type=pl.DeviceIdType.MESH)

    raw = jnp.concatenate([win_ref[...], emb_ref[...]], axis=0)
    left = raw - jnp.mean(raw, axis=1, keepdims=True)
    l3 = jnp.concatenate(split3(left), axis=0).astype(BF16)

    def folded(weights, width, db):
        got = contract(l3 if db == 0 else o3, weights, 1, db)
        return got[:width] + got[width:2 * width] + got[2 * width:3 * width]

    wot = wo_ref[...].T
    o3 = jnp.concatenate(split3(wot) + (jnp.zeros_like(wot),), axis=0).astype(BF16)
    root = math.sqrt(0.5)
    wbuf[0, 0:rank] = folded(wg_ref[...], rank, 0) * root
    wbuf[0, rank:2 * rank] = folded(wv_ref[...], rank, 0) * root
    wbuf[0, 2 * rank:2 * rank + lat] = folded(wd_ref[...], lat, 1)

    pl.semaphore_wait(barrier, n_tm + n_mp - 2)

    def table_copy(k):
        return pltpu.make_async_remote_copy(
            wbuf.at[0], wbuf.at[n_mp - k], wsend.at[k], wrecv.at[n_mp - k],
            device_id={"mp": lax.rem(mp + k, n_mp)}, device_id_type=pl.DeviceIdType.MESH)

    for k in range(1, n_mp):
        table_copy(k).start()

    def build(k):
        for part in range(2):
            a, b, c = split3(wbuf[k, part * rank:(part + 1) * rank])
            a_scr[k, part * units:(part + 1) * units] = jnp.concatenate([a, b, c, a, b, a], axis=0).T.astype(BF16)
        a, b, c = split3(wbuf[k, 2 * rank:2 * rank + lat])
        f_scr[k] = jnp.concatenate([a, b, c, jnp.zeros_like(a)], axis=0).astype(BF16)

    base = contract(wot, raw, 1, 1, precision=HIGH)
    rows = lax.broadcasted_iota(jnp.int32, (prompts, share), 0)
    for p in range(prompts):
        x = x_ref[p, 0, :, cols]
        u = jnp.concatenate([x, (rows == p).astype(F32)], axis=0)
        hc = contract(left, u, 0, 0, precision=HIGH)
        var = jnp.mean(hc * hc, axis=0, keepdims=True)
        y = u * lax.rsqrt(var + 1e-5)
        a, b, c = split3(y)
        y_scr[p] = jnp.concatenate([a, a, a, b, b, c], axis=0).astype(BF16)
        eps_ref[p, 0] = contract(base, u, 1, 0, precision=HIGH)

    def sweep(p, chunks, first):
        def body(t, _):
            at = pl.ds(pl.multiple_of(t * tile, 128), tile)
            yt = y_scr[p, :, at]
            total = jnp.zeros((4 * lat, tile), F32) if first else acc[:, at]
            for k in chunks:
                gate = jnp.dot(a_scr[k, :units], yt, preferred_element_type=F32)
                value = jnp.dot(a_scr[k, units:], yt, preferred_element_type=F32)
                hidden = ((gate * (1.0 + lax.erf(gate))) * value).astype(BF16)
                total = total + jnp.dot(f_scr[k], hidden, preferred_element_type=F32)
            acc[:, at] = total
            return 0

        lax.fori_loop(0, share // tile, body, 0)

    def drift_copy(p, k):
        to = lax.rem(tm + k, n_tm)
        return pltpu.make_async_remote_copy(
            dbuf.at[tm, p], dbuf.at[tm, p], dsend.at[k, p], drecv.at[tm, p],
            device_id={"tm": to}, device_id_type=pl.DeviceIdType.MESH)

    def drift_arrival(p, k):
        slot = lax.rem(tm + k, n_tm)
        return pltpu.make_async_remote_copy(
            dbuf.at[slot, p], dbuf.at[slot, p], dsend.at[k, p], drecv.at[slot, p],
            device_id={"tm": slot}, device_id_type=pl.DeviceIdType.MESH)

    def out_copy(p, k):
        return pltpu.make_async_remote_copy(
            out_ref.at[p, 0, :, cols], out_ref.at[p, 0, :, cols], osend.at[k, p], orecv.at[n_mp - k, p],
            device_id={"mp": lax.rem(mp + k, n_mp)}, device_id_type=pl.DeviceIdType.MESH)

    def out_arrival(p, k):
        peer = lax.rem(mp + k, n_mp)
        theirs = pl.ds(pl.multiple_of(peer * share, 128), share)
        return pltpu.make_async_remote_copy(
            out_ref.at[p, 0, :, theirs], out_ref.at[p, 0, :, theirs], osend.at[k, p], orecv.at[k, p],
            device_id={"mp": peer}, device_id_type=pl.DeviceIdType.MESH)

    def over_tm(op):
        lax.fori_loop(1, n_tm, lambda k, c: (op(k), c)[1], 0)

    def step(p):
        got = acc[...]
        eps = eps_ref[p, 0] + got[:lat] + got[lat:2 * lat] + got[2 * lat:3 * lat]
        eps_ref[p, 0] = eps
        x = x_ref[p, 0, :, cols]
        term = scal_ref[p, 0] * x - scal_ref[p, 1] * eps + scal_ref[p, 2] * z_ref[p, 0, :, cols]
        dbuf[tm, p] = term + jnp.where(tm == 0, 1.0, 0.0) * x
        over_tm(lambda k: drift_copy(p, k).start())

    def finish(p):
        over_tm(lambda k: drift_arrival(p, k).wait_recv())

        def add(j, total):
            return total + scal_ref[p, 3 + j] * dbuf[j, p]

        out_ref[p, 0, :, cols] = lax.fori_loop(0, n_tm, add, jnp.zeros((lat, share), F32))
        for k in range(1, n_mp):
            out_copy(p, k).start()

    build(0)
    sweep(0, (0,), True)
    for k in range(1, n_mp):
        table_copy(n_mp - k).wait_recv()
        build(k)
    sweep(0, range(1, n_mp), False)
    step(0)

    def lap(p, _):
        sweep(p, range(n_mp), True)
        step(p)
        finish(p - 1)
        return 0

    lax.fori_loop(1, prompts, lap, 0)
    finish(prompts - 1)
    for p in range(prompts):
        for k in range(1, n_mp):
            out_arrival(p, k).wait_recv()
    for k in range(1, n_mp):
        table_copy(k).wait_send()
        for p in range(prompts):
            out_copy(p, k).wait_send()
    for p in range(prompts):
        over_tm(lambda k: drift_copy(p, k).wait_send())


def shards(n_tm, n_mp, latents, noise, start_step, slide, w_in, w_gate, w_value, w_down, w_out):
    prompts, t_dev, lat, pos = latents.shape
    channels, units = w_gate.shape
    window = n_tm * t_dev
    share = pos // n_mp
    rank = lat + prompts
    assert t_dev == 1
    tm = lax.axis_index("tm")
    times = start_step - tm
    emb = embed(times.astype(F32), channels)
    grid = jnp.arange(TSTEPS, dtype=jnp.int32)
    hit = times[:, None] == grid
    coef = jnp.sum(jnp.where(hit[:, None, :], step_table()[None], 0.0), axis=-1)
    source = jnp.minimum(tm + slide, window - 1)
    keep = (jnp.arange(window, dtype=jnp.int32)[None, :] < source[:, None]).astype(F32)
    scal = jnp.concatenate([coef, keep], axis=1)
    vmem = pl.BlockSpec(memory_space=pltpu.VMEM)
    smem = pl.BlockSpec(memory_space=pltpu.SMEM)
    dma = pltpu.SemaphoreType.DMA
    return pl.pallas_call(
        functools.partial(kernel, n_tm, n_mp, 256),
        out_shape=(jax.ShapeDtypeStruct(latents.shape, F32), jax.ShapeDtypeStruct((prompts, 1, lat, share), F32)),
        in_specs=[vmem, vmem, vmem, smem, vmem, vmem, vmem, vmem, vmem],
        out_specs=(vmem, vmem),
        scratch_shapes=[
            pltpu.VMEM((n_mp, 2 * rank + 8, units), F32),
            pltpu.VMEM((n_mp, 2 * units, 6 * rank), BF16),
            pltpu.VMEM((n_mp, 4 * lat, units), BF16),
            pltpu.VMEM((prompts, 6 * rank, share), BF16),
            pltpu.VMEM((4 * lat, share), F32),
            pltpu.VMEM((n_tm, prompts, lat, share), F32),
            dma((n_mp,)), dma((n_mp,)),
            dma((n_tm, prompts)), dma((n_tm, prompts)),
            dma((n_mp, prompts)), dma((n_mp, prompts)),
        ],
        compiler_params=pltpu.CompilerParams(collective_id=0, has_side_effects=True, vmem_limit_bytes=60000 * 1024),
    )(latents, noise, emb, scal, w_in, w_gate, w_value, w_down, w_out)


def solution(mesh):
    in_specs = (
        P(None, "tm", None, None),
        P(None, "tm", None, None),
        P(),
        P(),
        P(),
        P(None, "mp"),
        P(None, "mp"),
        P("mp", None),
        P(),
    )
    out_specs = (P(None, "tm", None, None), P(None, "tm", None, "mp"))
    body = functools.partial(shards, mesh.shape["tm"], mesh.shape["mp"])
    return jax.shard_map(body, mesh=mesh, in_specs=in_specs, out_specs=out_specs, check_vma=False)
```

```python
import functools
import math

import jax
import jax.numpy as jnp
import numpy as np
from jax import lax
from jax.experimental import pallas as pl
from jax.experimental.pallas import tpu as pltpu
from jax.sharding import PartitionSpec as P

TSTEPS = 1000
F32, BF16 = jnp.float32, jnp.bfloat16
HIGH = lax.Precision.HIGHEST


def step_table(channels):
    beta = 1e-4 + (0.02 - 1e-4) * np.arange(TSTEPS, dtype=np.float64) / (TSTEPS - 1)
    abar = np.cumprod(1.0 - beta)
    root = np.sqrt(1.0 - beta)
    half = channels // 2
    freq = np.exp(-math.log(10000.0) * np.arange(half, dtype=np.float64) / half)
    table = np.zeros((4, max(TSTEPS, channels)), np.float32)
    table[:3, :TSTEPS] = [1.0 / root - 1.0, beta / np.sqrt(1.0 - abar) / root, np.sqrt(beta)]
    table[3, :channels] = np.concatenate([freq, freq])
    return table


def split3(v):
    a = v.astype(BF16).astype(F32)
    rest = v - a
    b = rest.astype(BF16).astype(F32)
    return a, b, rest - b


def six(parts, left):
    a, b, c = parts
    return jnp.concatenate([a, b, c, a, b, a] if left else [a, a, a, b, b, c], axis=0)


def contract(a, b, da, db, **kw):
    return lax.dot_general(a, b, (((da,), (db,)), ((), ())), preferred_element_type=F32, **kw)


def kernel(n_tm, n_mp, tile, x_hbm, z_hbm, start_ref, slide_ref, table_hbm, win_hbm, wg_hbm, wv_hbm, wd_hbm, wo_hbm,
           out_ref, eps_ref, x_ref, z_ref, table_ref, win_ref, wg_ref, wv_ref, wd_ref, wo_ref, load, hid, wbuf, a_scr, f_scr, y_scr, acc, dbuf, coef,
           wsend, wrecv, dsend, drecv, osend, orecv):
    prompts, _, lat, pos = x_hbm.shape
    units = wg_ref.shape[1]
    rank = lat + prompts
    share = pos // n_mp
    tm, mp = lax.axis_index("tm"), lax.axis_index("mp")
    cols = pl.ds(pl.multiple_of(mp * share, 128), share)

    pairs = [(win_hbm, win_ref), (table_hbm, table_ref), (wg_hbm, wg_ref), (wv_hbm, wv_ref), (wo_hbm, wo_ref),
             (wd_hbm, wd_ref), (x_hbm.at[:, :, :, cols], x_ref), (z_hbm.at[:, :, :, cols], z_ref)]
    loads = [pltpu.make_async_copy(a, b, load.at[i]) for i, (a, b) in enumerate(pairs)]
    for one in loads:
        one.start()
    barrier = pltpu.get_barrier_semaphore()

    def greet_tm(k, _):
        pl.semaphore_signal(barrier, inc=1, device_id={"tm": lax.rem(tm + k, n_tm)}, device_id_type=pl.DeviceIdType.MESH)
        return 0

    lax.fori_loop(1, n_tm, greet_tm, 0)
    for k in range(1, n_mp):
        pl.semaphore_signal(barrier, inc=1, device_id={"mp": lax.rem(mp + k, n_mp)}, device_id_type=pl.DeviceIdType.MESH)

    for one in loads[:6]:
        one.wait()
    channels = win_ref.shape[1]
    order = lax.broadcasted_iota(jnp.int32, (prompts, channels), 0)
    times = jnp.zeros((prompts, channels), F32)
    for p in range(prompts):
        times = jnp.where(order == p, (start_ref[p] - tm).astype(F32), times)
    angle = times * table_ref[3:4, :channels]
    lane = lax.broadcasted_iota(jnp.int32, (prompts, channels), 1)
    emb = jnp.where(lane < channels // 2, jnp.cos(angle), jnp.sin(angle))
    raw = jnp.concatenate([win_ref[...], emb], axis=0)
    left = raw - jnp.mean(raw, axis=1, keepdims=True)
    l3 = jnp.concatenate(split3(left), axis=0).astype(BF16)

    def folded(weights, width, db):
        got = contract(l3 if db == 0 else o3, weights, 1, db)
        return got[:width] + got[width:2 * width] + got[2 * width:3 * width]

    wot = wo_ref[...]
    o3 = jnp.concatenate(split3(wot) + (jnp.zeros_like(wot),), axis=0).astype(BF16)
    root = math.sqrt(0.5)
    wbuf[0, 0:rank] = folded(wg_ref[...], rank, 0) * root
    wbuf[0, rank:2 * rank] = folded(wv_ref[...], rank, 0) * root
    wbuf[0, 2 * rank:2 * rank + lat] = folded(wd_ref[...], lat, 1)

    pl.semaphore_wait(barrier, n_tm + n_mp - 2)

    def table_copy(k):
        return pltpu.make_async_remote_copy(
            wbuf.at[0], wbuf.at[n_mp - k], wsend.at[k], wrecv.at[n_mp - k],
            device_id={"mp": lax.rem(mp + k, n_mp)}, device_id_type=pl.DeviceIdType.MESH)

    for k in range(1, n_mp):
        table_copy(k).start()

    def build(k):
        for part in range(2):
            a, b, c = split3(wbuf[k, part * rank:(part + 1) * rank])
            a_scr[k, part * units:(part + 1) * units] = six((a, b, c), True).T.astype(BF16)
        a, b, c = split3(wbuf[k, 2 * rank:2 * rank + lat])
        f_scr[:, k * units:(k + 1) * units] = jnp.concatenate([a, b, c, jnp.zeros_like(a)], axis=0).astype(BF16)

    grid = lax.broadcasted_iota(jnp.int32, table_ref.shape, 1)
    for p in range(prompts):
        picked = jnp.where(grid == start_ref[p] - tm, table_ref[...], 0.0)
        coef[p] = jnp.broadcast_to(jnp.sum(picked, axis=1, keepdims=True), coef.shape[1:])

    base = contract(raw, wot, 1, 1, precision=HIGH)
    base6 = six(split3(base), True).T.astype(BF16)
    left6 = six(split3(left), True).T.astype(BF16)
    rows = lax.broadcasted_iota(jnp.int32, (prompts, share), 0)
    for one in loads[6:]:
        one.wait()
    for p in range(prompts):
        u = jnp.concatenate([x_ref[p, 0], (rows == p).astype(F32)], axis=0)
        u6 = six(split3(u), False).astype(BF16)
        hc = jnp.dot(left6, u6, preferred_element_type=F32)
        eps_ref[p, 0] = jnp.dot(base6, u6, preferred_element_type=F32)
        var = jnp.mean(hc * hc, axis=0, keepdims=True)
        y_scr[p] = six(split3(u * lax.rsqrt(var + 1e-5)), False).astype(BF16)

    def sweep(p, chunks, last):
        def body(t, _):
            at = pl.ds(pl.multiple_of(t * tile, 128), tile)
            yt = y_scr[p, :, at]
            for k in chunks:
                gate = jnp.dot(a_scr[k, :units], yt, preferred_element_type=F32)
                value = jnp.dot(a_scr[k, units:], yt, preferred_element_type=F32)
                hid[k * units:(k + 1) * units, at] = ((gate * (1.0 + lax.erf(gate))) * value).astype(BF16)
            if not last:
                return 0
            total = jnp.dot(f_scr[...], hid[:, at], preferred_element_type=F32)
            acc[:, at] = total
            return 0

        lax.fori_loop(0, share // tile, body, 0)

    def drift_copy(p, k):
        to = lax.rem(tm + k, n_tm)
        return pltpu.make_async_remote_copy(
            dbuf.at[tm, p], dbuf.at[tm, p], dsend.at[k, p], drecv.at[tm, p],
            device_id={"tm": to}, device_id_type=pl.DeviceIdType.MESH)

    def drift_arrival(p, k):
        slot = lax.rem(tm + k, n_tm)
        return pltpu.make_async_remote_copy(
            dbuf.at[slot, p], dbuf.at[slot, p], dsend.at[k, p], drecv.at[slot, p],
            device_id={"tm": slot}, device_id_type=pl.DeviceIdType.MESH)

    def out_copy(p, k):
        return pltpu.make_async_remote_copy(
            out_ref.at[p, 0, :, cols], out_ref.at[p, 0, :, cols], osend.at[k, p], orecv.at[n_mp - k, p],
            device_id={"mp": lax.rem(mp + k, n_mp)}, device_id_type=pl.DeviceIdType.MESH)

    def out_arrival(p, k):
        peer = lax.rem(mp + k, n_mp)
        theirs = pl.ds(pl.multiple_of(peer * share, 128), share)
        return pltpu.make_async_remote_copy(
            out_ref.at[p, 0, :, theirs], out_ref.at[p, 0, :, theirs], osend.at[k, p], orecv.at[k, p],
            device_id={"mp": peer}, device_id_type=pl.DeviceIdType.MESH)

    def over_tm(op):
        lax.fori_loop(1, n_tm, lambda k, c: (op(k), c)[1], 0)

    def step(p):
        got = acc[...]
        eps = eps_ref[p, 0] + got[:lat] + got[lat:2 * lat] + got[2 * lat:3 * lat]
        eps_ref[p, 0] = eps
        x = x_ref[p, 0]
        c = coef[p]
        term = c[0:1, :1] * x - c[1:2, :1] * eps + c[2:3, :1] * z_ref[p, 0]
        dbuf[tm, p] = term + jnp.where(tm == 0, 1.0, 0.0) * x
        over_tm(lambda k: drift_copy(p, k).start())

    def finish(p):
        over_tm(lambda k: drift_arrival(p, k).wait_recv())

        source = jnp.minimum(tm + slide_ref[p], n_tm - 1)

        def add(j, total):
            return total + jnp.where(j < source, 1.0, 0.0) * dbuf[j, p]

        out_ref[p, 0, :, cols] = lax.fori_loop(0, n_tm, add, jnp.zeros((lat, share), F32))
        for k in range(1, n_mp):
            out_copy(p, k).start()

    build(0)
    sweep(0, (0,), False)
    for k in range(1, n_mp):
        table_copy(n_mp - k).wait_recv()
        build(k)
    sweep(0, range(1, n_mp), True)
    step(0)

    def lap(p, _):
        sweep(p, range(n_mp), True)
        step(p)
        finish(p - 1)
        return 0

    lax.fori_loop(1, prompts, lap, 0)
    finish(prompts - 1)
    for p in range(prompts):
        for k in range(1, n_mp):
            out_arrival(p, k).wait_recv()
    for k in range(1, n_mp):
        table_copy(k).wait_send()
        for p in range(prompts):
            out_copy(p, k).wait_send()
    for p in range(prompts):
        over_tm(lambda k: drift_copy(p, k).wait_send())


def shards(n_tm, n_mp, latents, noise, start_step, slide, w_in, w_gate, w_value, w_down, w_out):
    prompts, t_dev, lat, pos = latents.shape
    channels, units = w_gate.shape
    share = pos // n_mp
    rank = lat + prompts
    assert t_dev == 1
    vmem = pl.BlockSpec(memory_space=pltpu.VMEM)
    smem = pl.BlockSpec(memory_space=pltpu.SMEM)
    dma = pltpu.SemaphoreType.DMA
    hbm = pl.BlockSpec(memory_space=pltpu.HBM)
    table = step_table(channels)
    return pl.pallas_call(
        functools.partial(kernel, n_tm, n_mp, 256),
        out_shape=(pltpu.VMEM(latents.shape, F32), pltpu.VMEM((prompts, 1, lat, share), F32)),
        in_specs=[hbm, hbm, smem, smem] + [hbm] * 6,
        out_specs=(vmem, vmem),
        scratch_shapes=[
            pltpu.VMEM((prompts, 1, lat, share), F32),
            pltpu.VMEM((prompts, 1, lat, share), F32),
            pltpu.VMEM(table.shape, F32),
            pltpu.VMEM(w_in.shape, F32),
            pltpu.VMEM(w_gate.shape, BF16),
            pltpu.VMEM(w_value.shape, BF16),
            pltpu.VMEM(w_down.shape, BF16),
            pltpu.VMEM(w_in.shape, F32),
            dma((8,)),
            pltpu.VMEM((n_mp * units, share), BF16),
            pltpu.VMEM((n_mp, 2 * rank + 8, units), F32),
            pltpu.VMEM((n_mp, 2 * units, 6 * rank), BF16),
            pltpu.VMEM((4 * lat, n_mp * units), BF16),
            pltpu.VMEM((prompts, 6 * rank, share), BF16),
            pltpu.VMEM((4 * lat, share), F32),
            pltpu.VMEM((n_tm, prompts, lat, share), F32),
            pltpu.VMEM((prompts, 4, 128), F32),
            dma((n_mp,)), dma((n_mp,)),
            dma((n_tm, prompts)), dma((n_tm, prompts)),
            dma((n_mp, prompts)), dma((n_mp, prompts)),
        ],
        compiler_params=pltpu.CompilerParams(collective_id=0, has_side_effects=True, vmem_limit_bytes=60000 * 1024),
    )(latents, noise, start_step, slide, table, w_in, w_gate, w_value, w_down, w_out.T)


def solution(mesh):
    in_specs = (
        P(None, "tm", None, None),
        P(None, "tm", None, None),
        P(),
        P(),
        P(),
        P(None, "mp"),
        P(None, "mp"),
        P("mp", None),
        P(),
    )
    out_specs = (P(None, "tm", None, None), P(None, "tm", None, "mp"))
    body = functools.partial(shards, mesh.shape["tm"], mesh.shape["mp"])
    return jax.shard_map(body, mesh=mesh, in_specs=in_specs, out_specs=out_specs, check_vma=False)
```

```python
import functools
import math

import jax
import jax.numpy as jnp
import numpy as np
from jax import lax
from jax.experimental import pallas as pl
from jax.experimental.pallas import tpu as pltpu
from jax.sharding import PartitionSpec as P

TSTEPS = 1000
F32, BF16 = jnp.float32, jnp.bfloat16
HIGH = lax.Precision.HIGHEST


def step_table(channels):
    beta = 1e-4 + (0.02 - 1e-4) * np.arange(TSTEPS, dtype=np.float64) / (TSTEPS - 1)
    abar = np.cumprod(1.0 - beta)
    root = np.sqrt(1.0 - beta)
    half = channels // 2
    freq = np.exp(-math.log(10000.0) * np.arange(half, dtype=np.float64) / half)
    table = np.zeros((4, max(TSTEPS, channels)), np.float32)
    table[:3, :TSTEPS] = [1.0 / root - 1.0, beta / np.sqrt(1.0 - abar) / root, np.sqrt(beta)]
    table[3, :channels] = np.concatenate([freq, freq])
    return table


def split3(v):
    a = v.astype(BF16).astype(F32)
    rest = v - a
    b = rest.astype(BF16).astype(F32)
    return a, b, rest - b


def six(parts, left):
    a, b, c = parts
    return jnp.concatenate([a, b, c, a, b, a] if left else [a, a, a, b, b, c], axis=0)


def contract(a, b, da, db, **kw):
    return lax.dot_general(a, b, (((da,), (db,)), ((), ())), preferred_element_type=F32, **kw)


def kernel(n_tm, n_mp, tile, x_hbm, z_hbm, start_ref, slide_ref, table_hbm, win_hbm, wg_hbm, wv_hbm, wd_hbm, wo_hbm,
           out_ref, eps_ref, x_ref, z_ref, table_ref, win_ref, wg_ref, wv_ref, wd_ref, wo_ref, load, hid, wbuf, a_scr, f_scr, y_scr, acc, dbuf, coef,
           wsend, wrecv, dsend, drecv, osend, orecv):
    prompts, _, lat, pos = x_hbm.shape
    units = wg_ref.shape[1]
    rank = lat + prompts
    share = pos // n_mp
    tm, mp = lax.axis_index("tm"), lax.axis_index("mp")
    cols = pl.ds(pl.multiple_of(mp * share, 128), share)

    pairs = [(win_hbm, win_ref), (table_hbm, table_ref), (wg_hbm, wg_ref), (wv_hbm, wv_ref), (wo_hbm, wo_ref),
             (wd_hbm, wd_ref), (x_hbm.at[:, :, :, cols], x_ref), (z_hbm.at[:, :, :, cols], z_ref)]
    loads = [pltpu.make_async_copy(a, b, load.at[i]) for i, (a, b) in enumerate(pairs)]
    for one in loads:
        one.start()
    barrier = pltpu.get_barrier_semaphore()

    def greet_tm(k, _):
        pl.semaphore_signal(barrier, inc=1, device_id={"tm": lax.rem(tm + k, n_tm)}, device_id_type=pl.DeviceIdType.MESH)
        return 0

    lax.fori_loop(1, n_tm, greet_tm, 0)
    for k in range(1, n_mp):
        pl.semaphore_signal(barrier, inc=1, device_id={"mp": lax.rem(mp + k, n_mp)}, device_id_type=pl.DeviceIdType.MESH)

    for one in loads[:6]:
        one.wait()
    channels = win_ref.shape[1]
    order = lax.broadcasted_iota(jnp.int32, (prompts, channels), 0)
    times = jnp.zeros((prompts, channels), F32)
    for p in range(prompts):
        times = jnp.where(order == p, (start_ref[p] - tm).astype(F32), times)
    angle = times * table_ref[3:4, :channels]
    lane = lax.broadcasted_iota(jnp.int32, (prompts, channels), 1)
    emb = jnp.where(lane < channels // 2, jnp.cos(angle), jnp.sin(angle))
    raw = jnp.concatenate([win_ref[...], emb], axis=0)
    left = raw - jnp.mean(raw, axis=1, keepdims=True)
    l3 = jnp.concatenate(split3(left), axis=0).astype(BF16)

    def folded(weights, width, db):
        got = contract(l3 if db == 0 else o3, weights, 1, db)
        return got[:width] + got[width:2 * width] + got[2 * width:3 * width]

    wot = wo_ref[...]
    o3 = jnp.concatenate(split3(wot) + (jnp.zeros_like(wot),), axis=0).astype(BF16)
    root = math.sqrt(0.5)
    wbuf[0, 0:rank] = folded(wg_ref[...], rank, 0) * root
    wbuf[0, rank:2 * rank] = folded(wv_ref[...], rank, 0) * root
    wbuf[0, 2 * rank:2 * rank + lat] = folded(wd_ref[...], lat, 1)

    pl.semaphore_wait(barrier, n_tm + n_mp - 2)

    def table_copy(k):
        return pltpu.make_async_remote_copy(
            wbuf.at[0], wbuf.at[n_mp - k], wsend.at[k], wrecv.at[n_mp - k],
            device_id={"mp": lax.rem(mp + k, n_mp)}, device_id_type=pl.DeviceIdType.MESH)

    for k in range(1, n_mp):
        table_copy(k).start()

    def build(k):
        for part in range(2):
            a, b, c = split3(wbuf[k, part * rank:(part + 1) * rank])
            a_scr[k, part * units:(part + 1) * units] = six((a, b, c), True).T.astype(BF16)
        a, b, c = split3(wbuf[k, 2 * rank:2 * rank + lat])
        f_scr[:, k * units:(k + 1) * units] = jnp.concatenate([a, b, c, jnp.zeros_like(a)], axis=0).astype(BF16)

    grid = lax.broadcasted_iota(jnp.int32, table_ref.shape, 1)
    for p in range(prompts):
        picked = jnp.where(grid == start_ref[p] - tm, table_ref[...], 0.0)
        coef[p] = jnp.broadcast_to(jnp.sum(picked, axis=1, keepdims=True), coef.shape[1:])

    base = contract(raw, wot, 1, 1, precision=HIGH)
    base6 = six(split3(base), True).T.astype(BF16)
    left6 = six(split3(left), True).T.astype(BF16)
    rows = lax.broadcasted_iota(jnp.int32, (prompts, share), 0)
    for one in loads[6:]:
        one.wait()
    for p in range(prompts):
        u = jnp.concatenate([x_ref[p, 0], (rows == p).astype(F32)], axis=0)
        u6 = six(split3(u), False).astype(BF16)
        hc = jnp.dot(left6, u6, preferred_element_type=F32)
        eps_ref[p, 0] = jnp.dot(base6, u6, preferred_element_type=F32)
        var = jnp.mean(hc * hc, axis=0, keepdims=True)
        y_scr[p] = six(split3(u * lax.rsqrt(var + 1e-5)), False).astype(BF16)

    def sweep(p, chunks, last):
        def body(t, _):
            at = pl.ds(pl.multiple_of(t * tile, 128), tile)
            yt = y_scr[p, :, at]
            for k in chunks:
                gate = jnp.dot(a_scr[k, :units], yt, preferred_element_type=F32)
                value = jnp.dot(a_scr[k, units:], yt, preferred_element_type=F32)
                hid[k * units:(k + 1) * units, at] = ((gate * (1.0 + lax.erf(gate))) * value).astype(BF16)
            if not last:
                return 0
            total = jnp.dot(f_scr[...], hid[:, at], preferred_element_type=F32)
            acc[:, at] = total
            return 0

        lax.fori_loop(0, share // tile, body, 0)

    def drift_copy(p, k):
        to = lax.rem(tm + k, n_tm)
        return pltpu.make_async_remote_copy(
            dbuf.at[tm, p], dbuf.at[tm, p], dsend.at[k, p], drecv.at[tm, p],
            device_id={"tm": to}, device_id_type=pl.DeviceIdType.MESH)

    def drift_arrival(p, k):
        slot = lax.rem(tm + k, n_tm)
        return pltpu.make_async_remote_copy(
            dbuf.at[slot, p], dbuf.at[slot, p], dsend.at[k, p], drecv.at[slot, p],
            device_id={"tm": slot}, device_id_type=pl.DeviceIdType.MESH)

    def out_copy(p, k):
        return pltpu.make_async_remote_copy(
            out_ref.at[p, 0, :, cols], out_ref.at[p, 0, :, cols], osend.at[k, p], orecv.at[n_mp - k, p],
            device_id={"mp": lax.rem(mp + k, n_mp)}, device_id_type=pl.DeviceIdType.MESH)

    def out_arrival(p, k):
        peer = lax.rem(mp + k, n_mp)
        theirs = pl.ds(pl.multiple_of(peer * share, 128), share)
        return pltpu.make_async_remote_copy(
            out_ref.at[p, 0, :, theirs], out_ref.at[p, 0, :, theirs], osend.at[k, p], orecv.at[k, p],
            device_id={"mp": peer}, device_id_type=pl.DeviceIdType.MESH)

    def over_tm(op):
        lax.fori_loop(1, n_tm, lambda k, c: (op(k), c)[1], 0)

    def step(p):
        got = acc[...]
        eps = eps_ref[p, 0] + got[:lat] + got[lat:2 * lat] + got[2 * lat:3 * lat]
        eps_ref[p, 0] = eps
        x = x_ref[p, 0]
        c = coef[p]
        term = c[0:1, :1] * x - c[1:2, :1] * eps + c[2:3, :1] * z_ref[p, 0]
        dbuf[tm, p] = term + jnp.where(tm == 0, 1.0, 0.0) * x
        over_tm(lambda k: drift_copy(p, k).start())

    def finish(p):
        over_tm(lambda k: drift_arrival(p, k).wait_recv())

        source = jnp.minimum(tm + slide_ref[p], n_tm - 1)

        def add(j, total):
            return total + jnp.where(j < source, 1.0, 0.0) * dbuf[j, p]

        out_ref[p, 0, :, cols] = lax.fori_loop(0, n_tm, add, jnp.zeros((lat, share), F32))
        for k in range(1, n_mp):
            out_copy(p, k).start()

    build(0)
    sweep(0, (0,), False)
    for k in range(1, n_mp):
        table_copy(n_mp - k).wait_recv()
        build(k)
    sweep(0, range(1, n_mp), True)
    step(0)

    def lap(p, _):
        sweep(p, range(n_mp), True)
        step(p)
        finish(p - 1)
        return 0

    lax.fori_loop(1, prompts, lap, 0)
    finish(prompts - 1)
    for p in range(prompts):
        for k in range(1, n_mp):
            out_arrival(p, k).wait_recv()
    for k in range(1, n_mp):
        table_copy(k).wait_send()
        for p in range(prompts):
            out_copy(p, k).wait_send()
    for p in range(prompts):
        over_tm(lambda k: drift_copy(p, k).wait_send())


def shards(n_tm, n_mp, latents, noise, start_step, slide, w_in, w_gate, w_value, w_down, w_out):
    prompts, t_dev, lat, pos = latents.shape
    channels, units = w_gate.shape
    share = pos // n_mp
    rank = lat + prompts
    assert t_dev == 1
    vmem = pl.BlockSpec(memory_space=pltpu.VMEM)
    smem = pl.BlockSpec(memory_space=pltpu.SMEM)
    dma = pltpu.SemaphoreType.DMA
    hbm = pl.BlockSpec(memory_space=pltpu.HBM)
    table = step_table(channels)
    return pl.pallas_call(
        functools.partial(kernel, n_tm, n_mp, 512),
        out_shape=(pltpu.VMEM(latents.shape, F32), pltpu.VMEM((prompts, 1, lat, share), F32)),
        in_specs=[hbm, hbm, smem, smem] + [hbm] * 6,
        out_specs=(vmem, vmem),
        scratch_shapes=[
            pltpu.VMEM((prompts, 1, lat, share), F32),
            pltpu.VMEM((prompts, 1, lat, share), F32),
            pltpu.VMEM(table.shape, F32),
            pltpu.VMEM(w_in.shape, F32),
            pltpu.VMEM(w_gate.shape, BF16),
            pltpu.VMEM(w_value.shape, BF16),
            pltpu.VMEM(w_down.shape, BF16),
            pltpu.VMEM(w_in.shape, F32),
            dma((8,)),
            pltpu.VMEM((n_mp * units, share), BF16),
            pltpu.VMEM((n_mp, 2 * rank + 8, units), F32),
            pltpu.VMEM((n_mp, 2 * units, 6 * rank), BF16),
            pltpu.VMEM((4 * lat, n_mp * units), BF16),
            pltpu.VMEM((prompts, 6 * rank, share), BF16),
            pltpu.VMEM((4 * lat, share), F32),
            pltpu.VMEM((n_tm, prompts, lat, share), F32),
            pltpu.VMEM((prompts, 4, 128), F32),
            dma((n_mp,)), dma((n_mp,)),
            dma((n_tm, prompts)), dma((n_tm, prompts)),
            dma((n_mp, prompts)), dma((n_mp, prompts)),
        ],
        compiler_params=pltpu.CompilerParams(collective_id=0, has_side_effects=True, vmem_limit_bytes=60000 * 1024),
    )(latents, noise, start_step, slide, table, w_in, w_gate, w_value, w_down, w_out.T)


def solution(mesh):
    in_specs = (
        P(None, "tm", None, None),
        P(None, "tm", None, None),
        P(),
        P(),
        P(),
        P(None, "mp"),
        P(None, "mp"),
        P("mp", None),
        P(),
    )
    out_specs = (P(None, "tm", None, None), P(None, "tm", None, "mp"))
    body = functools.partial(shards, mesh.shape["tm"], mesh.shape["mp"])
    return jax.shard_map(body, mesh=mesh, in_specs=in_specs, out_specs=out_specs, check_vma=False)
```
